256 devices in a mesh: grp: 32 (over y, x, core), rest: 8 (over z).
Axes of the slice: x: 4, y: 4, z: 8, core: 2. Of those that a mesh axis runs over, the one named last changes fastest.
Arguments:
- grads: bfloat16 [32, 18432, 1024], P('grp', 'rest'), parts along dimension 1, may hold values from -6 to 6
- weight: bfloat16 [18432, 1024], P('rest'), parts along dimension 0, may hold values from -0.625 to 0.625
- moment1: float32 [2304, 8192], P('grp', 'rest'), parts along dimension 1, may hold values from -2 to 2
- moment2: float32 [2304, 8192], P('grp', 'rest'), parts along dimension 1, may hold values from 0.0001 to 0.04
- step: int32 [1], replicated, may hold values from 1 to 8
Outputs:
- new_weight: bfloat16 [18432, 1024], P('rest'), parts along dimension 0
- new_moment1: float32 [2304, 8192], P('grp', 'rest'), parts along dimension 1
- new_moment2: float32 [2304, 8192], P('grp', 'rest'), parts along dimension 1
The draws below stay inside these ranges and needn't reach their ends.
There are 8 independent parts, one for each index of `rest`. The reference program is written for one: setup_inputs(seed, part) draws one part's arguments, and reference() takes and returns one part's arrays. A program takes and returns all parts, laid end to end along the dimension named above; an argument that names none is the same for every part. Nothing has to cross between parts.
All inputs are finite; a program needn't handle non-finite values.
Results may differ from the reference program's by a relative error of at most 0.006.
Values may be sent and summed in bfloat16 or wider, within the bound.
A program may use at most 128 MiB of HBM per device.

```python
import math
import jax
import jax.numpy as jnp
from jax import lax

D = 2304
KV = 1024
N_GRP = 32


def spiked(result, key, source, target, blocks, factor):
    owner, partner = [(jnp.arange(result.shape[position]) // (result.shape[position] // blocks)).reshape([-1 if axis == position else 1 for axis in range(result.ndim)]) for position in (source, target)]
    chosen = jax.random.permutation(key, blocks)[partner]
    strong = (owner == chosen) | (owner == (partner + blocks // 2) % blocks)
    return jnp.where(strong, factor * result, result)


def shard_levels(rng, dims, pieces, least, top_value):
    def one(position, blocks):
        steps = jax.random.uniform(jax.random.fold_in(jax.random.fold_in(rng, 6), position), (blocks,), jnp.float32, least / len(pieces), top_value / len(pieces))
        return jnp.repeat(jnp.exp(steps), dims[position] // blocks).reshape((-1,) + (1,) * (len(dims) - position - 1))

    loudness = one(*pieces[0])
    for cut in pieces[1:]:
        loudness = loudness * one(*cut)
    return loudness


def centred(stream_key, dims, spread, reach, cuts=(), dtype=jnp.bfloat16):
    drawn = spread * jax.random.normal(stream_key, dims, jnp.float32)
    if cuts:
        drawn = drawn * shard_levels(stream_key, dims, cuts, -0.22, 0.18)
    return jnp.clip(drawn, -reach, reach).astype(dtype)


def gaussian_with(stream_key, extent, deviation, reach, pieces, heavy, held_as=jnp.bfloat16):
    values = deviation * jax.random.normal(stream_key, extent, jnp.float32)
    if pieces:
        values = values * shard_levels(stream_key, extent, pieces, -0.22, 0.18)
    return jnp.clip(spiked(values, jax.random.fold_in(stream_key, 3), *heavy), -reach, reach).astype(held_as)


def setup_inputs(seed: int = 0, part: int = 0) -> dict:
    streams_of = jax.random.split(jax.random.key(seed), 6)
    own_keys = jax.random.split(jax.random.fold_in(streams_of[5], part), 6)
    return {
        "grads": gaussian_with(own_keys[0], (N_GRP, D, KV), 1.0, 6.0, ((0, 32),), (0, 1, 32, 2.75)),
        "weight": centred(own_keys[1], (D, KV), 0.04, 0.625),
        "moment1": centred(own_keys[2], (D, KV), 0.15, 2.0, ((0, 32),), jnp.float32),
        "moment2": jnp.clip(jnp.exp(math.log(0.04) - 5.9914646 * jax.random.uniform(own_keys[3], (D, KV), jnp.float32) ** shard_levels(own_keys[3], (D, KV), ((0, 32),), -0.2, 0.2)), 0.0001, 0.04),
        "step": jax.random.randint(streams_of[4], (1,), 1, 9).astype(jnp.int32),
    }


def reference(grads, weight, moment1, moment2, step):
    average = lax.optimization_barrier(jnp.sum(grads.astype(jnp.float32), axis=0)) / N_GRP
    new_moment1 = 0.9 * moment1 + 0.1 * average
    new_moment2 = 0.999 * moment2 + 0.001 * average * average
    step_count = step[0].astype(jnp.float32)
    first_hat = new_moment1 / (1.0 - jnp.power(jnp.float32(0.9), step_count))
    second_hat = new_moment2 / (1.0 - jnp.power(jnp.float32(0.999), step_count))
    updated = weight.astype(jnp.float32) * (1.0 - 0.25 * 0.1) - 0.25 * first_hat / (jnp.sqrt(second_hat) + 1e-08)
    return (updated.astype(jnp.bfloat16), new_moment1, new_moment2)
```

```python
import functools

import jax
import jax.numpy as jnp
import numpy as np
from jax import lax
from jax.experimental import pallas as pl
from jax.experimental.pallas import tpu as pltpu
from jax.sharding import PartitionSpec as P

SIDE = 4
CORES = 2
LANES = 128
PIECES = (192, 192, 192)

OFFSETS = (0, 1, 3, 2)
PLUS, MINUS = 0, 1


def sem_keys(pieces):
    keys = []
    for p in range(pieces):
        keys += [("D", p, j) for j in range(4)]
        keys += [(k, p, h) for k in ("A", "S", "B", "A2", "S2", "B2") for h in range(2)]
        keys += [(k, p, d) for k in ("GB", "FB") for d in range(2)]
        keys += [(k, p, d, q) for k in ("GA", "FA") for d in range(2) for q in range(4)]
        keys += [("P", p, da, q) for da in range(4) for q in range(4)]
    return {k: i for i, k in enumerate(keys)}


def powers(base, steps):
    base = float(np.float32(base))
    out = jnp.ones(steps.shape, jnp.float32)
    for k in range(31):
        out = jnp.where(((steps >> k) & 1) == 1, out * np.float32(base ** (2**k)), out)
    return out


def exchange_kernel(
    sizes, ids,
    step_ref, g_ref, w_ref, m1_ref, m2_ref,
    out, nm1, nm2,
    raw, rx, ra, rs, rb, ra2, rs2, rb2, wv, m1v, m2v,
    send_sems, recv_sems, load_sems,
):
    pieces = len(sizes)
    starts = [sum(sizes[:p]) for p in range(pieces)]
    g = lax.axis_index("grp")
    y, x, c = g // (SIDE * CORES), (g // CORES) % SIDE, g % CORES
    a = x * (1 - c) + y * c
    b = y * (1 - c) + x * c

    def at(da, db):
        ny = (y + da * c + db * (1 - c)) % SIDE
        nx = (x + da * (1 - c) + db * c) % SIDE
        return {"grp": (ny * SIDE + nx) * CORES + c}

    to_a = (at(1, 0), at(3, 0))
    to_b = (at(0, 1), at(0, 3))
    partner = {"grp": g + 1 - 2 * c}
    a_at = [(a + d) % SIDE for d in range(SIDE)]
    b_at = [(b + d) % SIDE for d in range(SIDE)]

    barrier = pltpu.get_barrier_semaphore()
    for device in (partner, *to_a, *to_b):
        pl.semaphore_signal(barrier, inc=1, device_id=device, device_id_type=pl.DeviceIdType.MESH)

    def rows(p, half=None):
        if half is None:
            return pl.ds(starts[p], sizes[p])
        return pl.ds(starts[p] + half * (sizes[p] // 2), sizes[p] // 2)

    def hrows(p):
        return pl.ds(starts[p] // 2, sizes[p] // 2)

    loads = []

    def load(src, dst):
        copy = pltpu.make_async_copy(src, dst, load_sems.at[len(loads)])
        copy.start()
        loads.append(copy)
        return copy

    piece_loads = []
    for p in range(pieces):
        mine = []
        for k in range(SIDE):
            mine.append(load(g_ref.at[:, k, 0, rows(p)], raw.at[0, k, :, rows(p)]))
            mine.append(load(g_ref.at[k, :, 1, rows(p)], raw.at[1, k, :, rows(p)]))
        piece_loads.append(mine)
    state_loads = [load(w_ref.at[y, x, c], wv), load(m1_ref, m1v), load(m2_ref, m2v)]

    sent = []

    def send(key, src, dst, device):
        copy = pltpu.make_async_remote_copy(
            src_ref=src, dst_ref=dst,
            send_sem=send_sems.at[ids[key]], recv_sem=recv_sems.at[ids[key]],
            device_id=device, device_id_type=pl.DeviceIdType.MESH,
        )
        copy.start()
        sent.append(copy)

    def arrived(key, dst, device):
        pltpu.make_async_remote_copy(
            src_ref=dst, dst_ref=dst,
            send_sem=send_sems.at[ids[key]], recv_sem=recv_sems.at[ids[key]],
            device_id=device, device_id_type=pl.DeviceIdType.MESH,
        ).wait_recv()

    pl.semaphore_wait(barrier, 5)

    for p in range(pieces):
        for copy in piece_loads[p]:
            copy.wait()
        for j, d in enumerate((2, 1, 3, 0)):
            send(("D", p, j), raw.at[1 - c, b_at[d], :, rows(p)], rx.at[b_at[d], :, rows(p)], partner)

    def each(body):
        def step(i, carry):
            body(i)
            return carry

        lax.fori_loop(0, SIDE, step, 0)

    def paired(p, j, d):
        arrived(("D", p, j), rx.at[a_at[d], :, rows(p)], partner)

        def body(i):
            raw[c, a_at[d], i, rows(p)] = raw[c, a_at[d], i, rows(p)] + rx[a_at[d], i, rows(p)]

        each(body)

    def f32(value):
        return value.astype(jnp.float32)

    def first_sends(p):
        paired(p, 0, 2)
        for h in range(2):
            send(("A", p, h), raw.at[c, a_at[2], :, rows(p, h)], ra.at[h, :, hrows(p)], to_a[h])
        paired(p, 1, 1)
        send(("S", p, 1), raw.at[c, a_at[1], :, rows(p, 1)], rs.at[1, :, hrows(p)], to_a[PLUS])
        paired(p, 2, 3)
        send(("S", p, 0), raw.at[c, a_at[3], :, rows(p, 0)], rs.at[0, :, hrows(p)], to_a[MINUS])
        paired(p, 3, 0)

    def first_relay(p):
        for h in range(2):
            far = a_at[1 + 2 * h]
            arrived(("A", p, h), ra.at[h, :, hrows(p)], to_a[h])

            def body(i):
                raw[c, far, i, rows(p, h)] = raw[c, far, i, rows(p, h)] + ra[h, i, hrows(p)]

            each(body)
            send(("B", p, h), raw.at[c, far, :, rows(p, h)], rb.at[h, :, hrows(p)], to_a[h])

    def second_sends(p):
        for h in range(2):
            arrived(("S", p, h), rs.at[h, :, hrows(p)], to_a[h])
        for h in range(2):
            arrived(("B", p, h), rb.at[h, :, hrows(p)], to_a[h])

            def body(i):
                total = f32(raw[c, a, i, rows(p, h)]) + f32(rs[h, i, hrows(p)]) + f32(rb[h, i, hrows(p)])
                raw[c, a, i, rows(p, h)] = total.astype(jnp.bfloat16)

            each(body)
        for h in range(2):
            send(("A2", p, h), raw.at[c, a, b_at[2], rows(p, h)], ra2.at[h, hrows(p)], to_b[h])
        send(("S2", p, 1), raw.at[c, a, b_at[1], rows(p, 1)], rs2.at[1, hrows(p)], to_b[PLUS])
        send(("S2", p, 0), raw.at[c, a, b_at[3], rows(p, 0)], rs2.at[0, hrows(p)], to_b[MINUS])

    def second_relay(p):
        for h in range(2):
            far = b_at[1 + 2 * h]
            arrived(("A2", p, h), ra2.at[h, hrows(p)], to_b[h])
            raw[c, a, far, rows(p, h)] = raw[c, a, far, rows(p, h)] + ra2[h, hrows(p)]
            send(("B2", p, h), raw.at[c, a, far, rows(p, h)], rb2.at[h, hrows(p)], to_b[h])

    steps = jnp.full((8, LANES), step_ref[0], jnp.int32)
    scale1 = (1.0 / (1.0 - powers(0.9, steps)))[0:1]
    scale2 = (1.0 / (1.0 - powers(0.999, steps)))[0:1]

    def update(p):
        if p == 0:
            for copy in state_loads:
                copy.wait()
        for h in range(2):
            arrived(("S2", p, h), rs2.at[h, hrows(p)], to_b[h])
        for h in range(2):
            arrived(("B2", p, h), rb2.at[h, hrows(p)], to_b[h])
            r = rows(p, h)
            total = f32(raw[c, a, b, r]) + f32(rs2[h, hrows(p)]) + f32(rb2[h, hrows(p)])
            average = total * (1.0 / (SIDE * SIDE * CORES))
            moment1 = 0.9 * m1v[r] + 0.1 * average
            moment2 = 0.999 * m2v[r] + 0.001 * average * average
            nm1[r] = moment1
            nm2[r] = moment2
            change = 0.25 * (moment1 * scale1) / (jnp.sqrt(moment2 * scale2) + 1e-08)
            out[c, a, b, r] = (f32(wv[r]) * (1.0 - 0.25 * 0.1) - change).astype(jnp.bfloat16)
        own = out.at[c, a, b, rows(p)]
        for d in range(2):
            send(("GB", p, d), own, own, to_b[d])
        spread(p, 0)

    def to_partner(p, da, q):
        block = out.at[c, a_at[da], b_at[OFFSETS[q]], rows(p)]
        send(("P", p, da, q), block, block, partner)

    def spread(p, q):
        block = out.at[c, a, b_at[OFFSETS[q]], rows(p)]
        for d in range(2):
            send(("GA", p, d, q), block, block, to_a[d])
        to_partner(p, 0, q)

    def second_gather(p):
        for d in range(2):
            back = b_at[3 - 2 * d]
            arrived(("GB", p, d), out.at[c, a, back, rows(p)], to_b[d])
            half = out.at[c, a, back, rows(p, d)]
            send(("FB", p, d), half, half, to_b[d])
        spread(p, 1)
        spread(p, 2)

    def second_done(p):
        for d in range(2):
            arrived(("FB", p, d), out.at[c, a, b_at[2], rows(p, d)], to_b[d])
        spread(p, 3)
        relay(p, 0)

    def relay(p, q):
        for d in range(2):
            back = 3 - 2 * d
            arrived(("GA", p, d, q), out.at[c, a_at[back], b_at[OFFSETS[q]], rows(p)], to_a[d])
            half = out.at[c, a_at[back], b_at[OFFSETS[q]], rows(p, d)]
            send(("FA", p, d, q), half, half, to_a[d])
            to_partner(p, back, q)

    def landed(p, q):
        for d in range(2):
            arrived(("FA", p, d, q), out.at[c, a_at[2], b_at[OFFSETS[q]], rows(p, d)], to_a[d])
        to_partner(p, 2, q)

    def first_gather(p):
        relay(p, 1)
        relay(p, 2)
        landed(p, 0)

    def first_tail(p):
        relay(p, 3)
        landed(p, 1)
        landed(p, 2)

    def first_done(p):
        landed(p, 3)

    stages = (
        first_sends, first_relay, second_sends, second_relay, update,
        second_gather, second_done, first_gather, first_tail, first_done,
    )
    for slot in range(len(stages) + pieces - 1):
        for p in range(pieces):
            if 0 <= slot - p < len(stages):
                stages[slot - p](p)

    for p in range(pieces):
        for da in range(4):
            for q in range(4):
                arrived(("P", p, da, q), out.at[1 - c, b_at[da], a_at[OFFSETS[q]], rows(p)], partner)
    for copy in sent:
        copy.wait_send()


def store_kernel(out, nm1, nm2, w_ref, m1_ref, m2_ref, sems):
    copies = []

    def store(src, dst):
        copy = pltpu.make_async_copy(src, dst, sems.at[len(copies)])
        copy.start()
        copies.append(copy)

    for k in range(SIDE):
        store(out.at[0, k], w_ref.at[:, k, 0])
        store(out.at[1, k], w_ref.at[k, :, 1])
    store(nm1, m1_ref)
    store(nm2, m2_ref)
    for copy in copies:
        copy.wait()


def tiled(array):
    rows, columns = array.shape
    parts = array.reshape(rows // 8, 8, columns // LANES, LANES)
    return parts.transpose(0, 2, 1, 3).reshape(rows * columns // LANES, LANES)


def untiled(array, rows, columns):
    parts = array.reshape(rows // 8, columns // LANES, 8, LANES)
    return parts.transpose(0, 2, 1, 3).reshape(rows, columns)


def shards(grads, weight, moment1, moment2, step):
    own, columns = moment1.shape
    depth = own * columns // LANES
    grid = (SIDE, SIDE, CORES, depth, LANES)
    sizes = PIECES
    ids = sem_keys(len(sizes))
    bf16 = jnp.bfloat16
    vmem = pl.BlockSpec(memory_space=pltpu.VMEM)
    hbm = pl.BlockSpec(memory_space=pltpu.HBM)
    out, nm1, nm2 = pl.pallas_call(
        functools.partial(exchange_kernel, sizes, ids),
        out_shape=(
            pltpu.VMEM((CORES, SIDE, SIDE, depth, LANES), bf16),
            pltpu.VMEM((depth, LANES), jnp.float32),
            pltpu.VMEM((depth, LANES), jnp.float32),
        ),
        in_specs=[pl.BlockSpec(memory_space=pltpu.SMEM)] + [hbm] * 4,
        out_specs=(vmem,) * 3,
        scratch_shapes=[
            pltpu.VMEM((CORES, SIDE, SIDE, depth, LANES), bf16),
            pltpu.VMEM((SIDE, SIDE, depth, LANES), bf16),
            *[pltpu.VMEM((2, SIDE, depth // 2, LANES), bf16)] * 3,
            *[pltpu.VMEM((2, depth // 2, LANES), bf16)] * 3,
            pltpu.VMEM((depth, LANES), bf16),
            *[pltpu.VMEM((depth, LANES), jnp.float32)] * 2,
            pltpu.SemaphoreType.DMA((len(ids),)),
            pltpu.SemaphoreType.DMA((len(ids),)),
            pltpu.SemaphoreType.DMA((8 * len(sizes) + 3,)),
        ],
        compiler_params=pltpu.CompilerParams(collective_id=0, has_side_effects=True, vmem_limit_bytes=40 << 20),
        name="reduce_update_gather",
    )(step, *(
        pltpu.with_memory_space_constraint(array, pltpu.HBM)
        for array in (
            tiled(grads[0]).reshape(grid), tiled(weight).reshape(grid), tiled(moment1), tiled(moment2)
        )
    ))
    new_weight, new_moment1, new_moment2 = pl.pallas_call(
        store_kernel,
        out_shape=(
            jax.ShapeDtypeStruct(grid, bf16),
            jax.ShapeDtypeStruct((depth, LANES), jnp.float32),
            jax.ShapeDtypeStruct((depth, LANES), jnp.float32),
        ),
        in_specs=[vmem] * 3,
        out_specs=(hbm,) * 3,
        scratch_shapes=[pltpu.SemaphoreType.DMA((2 * SIDE + 2,))],
        compiler_params=pltpu.CompilerParams(vmem_limit_bytes=1 << 20),
        name="store",
    )(*(pltpu.with_memory_space_constraint(array, pltpu.VMEM) for array in (out, nm1, nm2)))
    return (
        untiled(new_weight.reshape(-1, LANES), *weight.shape),
        untiled(new_moment1, own, columns),
        untiled(new_moment2, own, columns),
    )


def solution(mesh):
    return jax.shard_map(
        shards,
        mesh=mesh,
        in_specs=(P("grp", "rest", None), P("rest", None), P("grp", "rest"), P("grp", "rest"), P()),
        out_specs=(P("rest", None), P("grp", "rest"), P("grp", "rest")),
        check_vma=False,
    )
```
